32 devices in a mesh: band: 16 (over z, y, core), sub: 2 (over x).
Axes of the slice: x: 2, y: 2, z: 4, core: 2. Of those that a mesh axis runs over, the one named last changes fastest.
Arguments:
- land_values: bfloat16 [64, 524288], P(None, ('band', 'sub')), may hold values from -6 to 6
- area_weights: bfloat16 [4096, 128, 128], P(('band', 'sub')), may hold values from 0.0019989014 to 0.029907227
- land_mask: int32 [524288], P(('band', 'sub')), may hold values 0 or 1
- dest_band: int32 [4096, 1], P(('band', 'sub')), may hold values from 0 to 15; in each aligned block of 128 rows (0 to 127, 128 to 255, ...) at most 16 rows name the same one
- dest_tile: int32 [4096], P(('band', 'sub')), may hold values from 0 to 399
- ocean_mask: int32 [819200], P(('band', 'sub')), may hold values 0 or 1
Outputs:
- remapped: float32 [64, 819200], P(None, ('band', 'sub'))
The draws below stay inside these ranges and needn't reach their ends.
Inputs may be any that keep to these rules, and one draw needn't show every extreme that they name: `dest_band`: each device's 128 blocks name any one band at most 16 times; in every draw some device names one band exactly 16 times.
All inputs are finite; a program needn't handle non-finite values. No bound on the sum of `land_mask` or of `ocean_mask` on one device may be relied on, other than what follows from the above.
Results may differ from the reference program's by a relative error of at most 0.005.
Values may be sent and summed in bfloat16 or wider, within the bound.
A program may use at most 128 MiB of HBM per device.

```python
import math
import jax
import jax.numpy as jnp
import numpy as np
from jax import lax

F = 64
BL = 128
OT = 128
LB_DEV = 128
CAP = 16
TILES_BAND = 400
NBLK = 4096
NLAND = 524288
NOCN = 819200
N_BAND = 16


def touch_ends(result, rng, low, largest):
    longest = result.shape.index(max(result.shape))
    spots = []
    for shift in (0, 1):
        where = [jax.random.randint(jax.random.fold_in(rng, axis), (), 0, length) for axis, length in enumerate(result.shape)]
        where[longest] = (where[longest] + shift) % result.shape[longest]
        spots.append(tuple(where))
    return result.at[spots[0]].set(low).at[spots[1]].set(largest)


def level_of(stream_key, shape, split, least, largest):
    def one(position, shards_of):
        draws = jax.random.uniform(jax.random.fold_in(jax.random.fold_in(stream_key, 6), position), (shards_of,), jnp.float32, least / len(split), largest / len(split))
        return jnp.repeat(jnp.exp(draws), shape[position] // shards_of).reshape((-1,) + (1,) * (len(shape) - position - 1))

    gain = one(*split[0])
    for cut in split[1:]:
        gain = gain * one(*cut)
    return gain


def shared_out(own_key, own, number, rows, number_of, top, bound, lean):
    sequence = jax.random.permutation(own_key, number_of)
    packed, common = load_shares(number_of, rows * top, bound, lean, True), load_shares(number_of, rows * top, bound, lean, False)
    places = jnp.arange(number_of)

    def named(tallies, offset_by):
        used = int((tallies > 0).sum())
        fixed = max(1, used // 4)
        shifted = fixed + (places - fixed + offset_by * (used - fixed)) % max(1, number_of - fixed)
        return jnp.zeros((number_of,), jnp.int32).at[sequence[jnp.where(places < fixed, places, shifted)]].set(jnp.asarray(tallies, jnp.int32))

    tallies = jnp.where(number % 4 == 0, named(packed, number // 4), named(common, number - number // 4 - 1))
    mixed = jax.random.permutation(jax.random.fold_in(own, 3), number_of)
    donor, sink = mixed[0:number_of // 2 * 2:2], mixed[1:number_of // 2 * 2:2]
    room = jnp.minimum(tallies[donor] - 1, bound - tallies[sink]) // 2
    room = jnp.where((donor == sequence[0]) | (sink == sequence[0]) | (tallies[sink] == 0), 0, jnp.maximum(room, 0))
    shifted = jax.random.randint(jax.random.fold_in(own, 4), (number_of // 2,), 0, 1 << 20) % (room + 1)
    tallies = tallies.at[donor].add(-shifted).at[sink].add(shifted)
    labels = jnp.searchsorted(jnp.cumsum(tallies), jnp.arange(rows * top), side="right").astype(jnp.int32)
    listing = labels.reshape(top, rows).T
    listing = listing[jax.random.permutation(jax.random.fold_in(own, 1), rows)]
    offset_by = jax.random.randint(jax.random.fold_in(own, 2), (rows, 1), 0, top)
    return jnp.take_along_axis(listing, (jnp.arange(top)[None, :] + offset_by) % top, axis=1)


def load_shares(count, total, reach, lean, full):
    loads = [(1 << 20) // math.isqrt(rank ** lean) + 1 for rank in range(1, count + 1)]
    largest = reach if full else min(reach, max(-(-total // count), total * loads[0] // sum(loads)))
    least = 1 if total - largest >= count - 1 else 0
    given, surplus = [largest] + [least] * (count - 1), total - largest - least * (count - 1)
    while surplus > 0:
        free = [i for i in range(1, count) if given[i] < largest] or [i for i in range(1, count) if given[i] < reach]
        pool, budget = sum([loads[i] for i in free]), surplus
        for i in free:
            more = min(reach - given[i], max(1, budget * loads[i] // pool), surplus)
            given[i] = given[i] + more
            surplus = surplus - more
    return np.array(given)


def gaussian(stream_key, dims, spread, most, shards=(), dtype=jnp.bfloat16):
    drawn = jax.random.normal(stream_key, dims, jnp.float32) * spread
    if len(shards) > 0:
        drawn = level_of(stream_key, dims, shards, -0.22, 0.18) * drawn
    return jnp.clip(drawn, min=-most, max=most).astype(dtype)


def setup_inputs(seed: int = 0) -> dict:
    key_of = jax.random.split(jax.random.key(seed), 7)
    land_values = gaussian(key_of[0], (F, NLAND), 1.0, 6.0, ((1, 32),))
    area_weights = jnp.clip(jnp.exp(math.log(0.029907227) - 2.7055024 * jax.random.uniform(key_of[1], (NBLK, BL, OT), jnp.float32) ** level_of(key_of[1], (NBLK, BL, OT), ((0, 32),), -0.2, 0.2)), 0.0019989014, 0.029907227).astype(jnp.bfloat16)
    land_mask = touch_ends((jax.random.randint(key_of[2], (NLAND,), 0, 2) < 1).astype(jnp.int32), jax.random.fold_in(key_of[2], 1), 0, 1)
    dest_band_keys = jax.random.split(jax.random.fold_in(key_of[3], 1), NBLK // LB_DEV)
    dest_band_turns = jax.random.permutation(jax.random.fold_in(key_of[3], 3), NBLK // LB_DEV)
    dest_band = jax.vmap(lambda own, number: shared_out(jax.random.fold_in(key_of[3], 2), own, number, LB_DEV, N_BAND, 1, CAP, 2))(dest_band_keys, dest_band_turns).reshape((NBLK, 1))
    dest_tile = touch_ends(jax.random.randint(key_of[4], (NBLK,), 0, TILES_BAND), jax.random.fold_in(key_of[4], 1), 0, TILES_BAND - 1).astype(jnp.int32)
    ocean_mask = touch_ends((jax.random.randint(key_of[5], (NOCN,), 0, 4) < 3).astype(jnp.int32), jax.random.fold_in(key_of[5], 1), 0, 1)
    return dict(land_values=land_values, area_weights=area_weights, land_mask=land_mask, dest_band=dest_band, dest_tile=dest_tile, ocean_mask=ocean_mask)


cover_floor = 0.5


def reference(land_values, area_weights, land_mask, dest_band, dest_tile, ocean_mask):
    groups = area_weights.shape[0] // LB_DEV
    tiles_all = N_BAND * TILES_BAND
    block_values = land_values.reshape(F, groups, LB_DEV, BL).transpose(1, 2, 0, 3)
    block_weights = area_weights.reshape(groups, LB_DEV, BL, OT)
    block_masks = land_mask.reshape(groups, LB_DEV, BL)
    block_tiles = (dest_band[:, 0] * TILES_BAND + dest_tile).astype(jnp.int32).reshape(groups, LB_DEV)

    def remap_group(carry, inputs):
        summed, coverage = carry
        values, weights, masks, tiles = inputs
        masked = weights * masks.astype(jnp.bfloat16)[:, :, None]
        partial_value = jnp.einsum("bfl,blo->bfo", values.astype(jnp.float32), masked.astype(jnp.float32)).astype(jnp.bfloat16)
        covered = jnp.sum(masked.astype(jnp.float32), axis=1).astype(jnp.bfloat16)
        summed = summed.at[:, tiles].add(jnp.transpose(partial_value.astype(jnp.float32), (1, 0, 2)))
        coverage = coverage.at[tiles].add(covered.astype(jnp.float32))
        return (summed, coverage), None

    start_state = (jnp.zeros((F, tiles_all, OT), jnp.float32), jnp.zeros((tiles_all, OT), jnp.float32))
    (summed, coverage), unused = lax.scan(remap_group, start_state, (block_values, block_weights, block_masks, block_tiles))
    ocean_keep = ocean_mask.reshape(tiles_all, OT).astype(jnp.float32)
    remapped = summed * ocean_keep[None] / jnp.maximum(coverage, cover_floor)[None]
    return remapped.reshape(F, tiles_all * OT)
```

```python
import functools

import jax
import jax.numpy as jnp
from jax import lax
from jax.experimental import pallas as pl
from jax.experimental.pallas import tpu as pltpu
from jax.sharding import PartitionSpec as P

cover_floor = 0.5
ROWS = 16


def block_kernel(group, chunks, v_ref, w_ref, m_ref, p_ref, c_ref):
    cells = w_ref.shape[1]
    for j in range(group):
        lanes = pl.ds(j * cells, cells)
        m = m_ref[:, lanes].astype(jnp.float32)
        mb = m.astype(jnp.bfloat16)
        lhs = jnp.concatenate(
            [v_ref[:, lanes] * mb, jnp.broadcast_to(mb, (ROWS, cells))], axis=0
        )
        p = jnp.dot(lhs, w_ref[j], preferred_element_type=jnp.float32)
        for c in range(chunks):
            p_ref[c, j] = p[c * ROWS:(c + 1) * ROWS].astype(jnp.bfloat16)
        c_ref[pl.ds(j, 1), :] = (
            p[chunks * ROWS:chunks * ROWS + 1].astype(jnp.bfloat16).astype(jnp.float32)
        )


def block_products(values, weights, mask):
    fields = values.shape[0]
    blocks, cells, out_cells = weights.shape
    chunks = fields // ROWS
    group = 16
    return pl.pallas_call(
        functools.partial(block_kernel, group, chunks),
        grid=(blocks // group,),
        in_specs=[
            pl.BlockSpec((fields, group * cells), lambda i: (0, i)),
            pl.BlockSpec((group, cells, out_cells), lambda i: (i, 0, 0)),
            pl.BlockSpec((1, group * cells), lambda i: (0, i)),
        ],
        out_specs=[
            pl.BlockSpec((chunks, group, ROWS, out_cells), lambda i: (0, i, 0, 0)),
            pl.BlockSpec((group, out_cells), lambda i: (i, 0)),
        ],
        out_shape=[
            jax.ShapeDtypeStruct((chunks, blocks, ROWS, out_cells), jnp.bfloat16),
            jax.ShapeDtypeStruct((blocks, out_cells), jnp.float32),
        ],
        name="block_products",
        cost_estimate=pl.CostEstimate(
            flops=2 * blocks * fields * cells * out_cells,
            bytes_accessed=8 * 1024 * 1024,
            transcendentals=0,
        ),
    )(values, weights, mask)


def exchange_kernel(
    bands, cap, chunks, tiles,
    src_ref, prev_ref, last_ref, p_ref, c_ref, keep_ref, out_ref,
    send, recv, csend, crecv, run, crun, xsend, xrecv, cxsend, cxrecv,
    send_sem, recv_sem, csend_sem, crecv_sem, xsend_sem, xrecv_sem,
):
    me = lax.axis_index("band")
    half = lax.axis_index("sub")
    slots = bands * cap
    other = {"sub": 1 - half}

    barrier = pltpu.get_barrier_semaphore()

    @pl.loop(1, bands)
    def _(k):
        pl.semaphore_signal(
            barrier, inc=1, device_id={"band": lax.rem(me + k, bands)},
            device_id_type=pl.DeviceIdType.MESH,
        )

    pl.semaphore_signal(barrier, inc=1, device_id=other, device_id_type=pl.DeviceIdType.MESH)
    pl.semaphore_wait(barrier, bands)

    def chunk_copy(c, d, source):
        return pltpu.make_async_remote_copy(
            src_ref=send.at[c, d], dst_ref=recv.at[c, source],
            send_sem=send_sem.at[c, d], recv_sem=recv_sem.at[c, source],
            device_id={"band": d}, device_id_type=pl.DeviceIdType.MESH,
        )

    def cover_copy(d, source):
        return pltpu.make_async_remote_copy(
            src_ref=csend.at[d], dst_ref=crecv.at[source],
            send_sem=csend_sem.at[d], recv_sem=crecv_sem.at[source],
            device_id={"band": d}, device_id_type=pl.DeviceIdType.MESH,
        )

    def half_copy(c):
        return pltpu.make_async_remote_copy(
            src_ref=xsend.at[c], dst_ref=xrecv.at[c],
            send_sem=xsend_sem.at[c], recv_sem=xrecv_sem.at[c],
            device_id=other, device_id_type=pl.DeviceIdType.MESH,
        )

    half_cover = pltpu.make_async_remote_copy(
        src_ref=cxsend, dst_ref=cxrecv,
        send_sem=xsend_sem.at[chunks], recv_sem=xrecv_sem.at[chunks],
        device_id=other, device_id_type=pl.DeviceIdType.MESH,
    )

    @pl.loop(1, bands)
    def _(k):
        d = lax.rem(me + k, bands)
        for j in range(cap):
            csend[d, pl.ds(j, 1), :] = c_ref[pl.ds(src_ref[d * cap + j], 1), :]
        cover_copy(d, me).start()

    for j in range(cap):
        crecv[me, pl.ds(j, 1), :] = c_ref[pl.ds(src_ref[me * cap + j], 1), :]

    for c in range(chunks):
        @pl.loop(1, bands)
        def _(k, c=c):
            d = lax.rem(me + k, bands)
            for j in range(cap):
                send[c, d, j] = p_ref[c, src_ref[d * cap + j]]
            chunk_copy(c, d, me).start()

        for j in range(cap):
            recv[c, me, j] = p_ref[c, src_ref[me * cap + j]]

    @pl.loop(1, bands)
    def _(k):
        cover_copy(me, lax.rem(me + k, bands)).wait_recv()

    crun[pl.ds(slots, 8), :] = jnp.zeros((8, crun.shape[1]), jnp.float32)

    @pl.loop(0, bands)
    def _(s):
        for j in range(cap):
            i = s * cap + j
            crun[pl.ds(i, 1), :] = (
                crun[pl.ds(prev_ref[i], 1), :] + crecv[s, pl.ds(j, 1), :]
            )

    step = 8

    @pl.loop(0, tiles // step)
    def _(g):
        for u in range(step):
            t = g * step + u
            cxsend[pl.ds(t, 1), :] = crun[pl.ds(last_ref[t], 1), :]

    half_cover.start()

    for c in range(chunks):
        @pl.loop(1, bands)
        def _(k, c=c):
            chunk_copy(c, me, lax.rem(me + k, bands)).wait_recv()

        run[c, slots] = jnp.zeros(run.shape[2:], jnp.float32)

        @pl.loop(0, bands)
        def _(s, c=c):
            for j in range(cap):
                i = s * cap + j
                run[c, i] = run[c, prev_ref[i]] + recv[c, s, j].astype(jnp.float32)

        @pl.loop(0, tiles // step)
        def _(g, c=c):
            for u in range(step):
                t = g * step + u
                xsend[c, t] = run[c, last_ref[t]].astype(jnp.bfloat16)

        half_copy(c).start()

    half_cover.wait_recv()

    @pl.loop(0, tiles // step)
    def _(g):
        for u in range(step):
            t = g * step + u
            row = pl.ds(t, 1)
            total = crun[pl.ds(last_ref[tiles + t], 1), :] + cxrecv[row, :]
            cxrecv[row, :] = keep_ref[row, :] / jnp.maximum(total, cover_floor)

    cells = xsend.shape[3]
    for c in range(chunks):
        half_copy(c).wait_recv()

        @pl.loop(0, tiles // step)
        def _(g, c=c):
            for u in range(step):
                t = g * step + u
                total = run[c, last_ref[tiles + t]] + xrecv[c, t].astype(jnp.float32)
                lanes = pl.ds(pl.multiple_of(t * cells, cells), cells)
                out_ref[pl.ds(c * ROWS, ROWS), lanes] = total * cxrecv[pl.ds(t, 1), :]

    half_cover.wait_send()
    for c in range(chunks):
        half_copy(c).wait_send()

    @pl.loop(1, bands)
    def _(k):
        d = lax.rem(me + k, bands)
        cover_copy(d, me).wait_send()
        for c in range(chunks):
            chunk_copy(c, d, me).wait_send()


def exchange(bands, cap, src, prev, last, partial, covered, keep):
    chunks, _, rows, cells = partial.shape
    tiles = keep.shape[0]
    slots = bands * cap
    smem = pl.BlockSpec(memory_space=pltpu.SMEM)
    vmem = pl.BlockSpec(memory_space=pltpu.VMEM)
    bf16, f32 = jnp.bfloat16, jnp.float32
    dma = pltpu.SemaphoreType.DMA
    return pl.pallas_call(
        functools.partial(exchange_kernel, bands, cap, chunks, tiles),
        in_specs=[smem, smem, smem, vmem, vmem, vmem],
        out_specs=vmem,
        out_shape=jax.ShapeDtypeStruct((chunks * rows, tiles * cells), f32),
        scratch_shapes=[
            pltpu.VMEM((chunks, bands, cap, rows, cells), bf16),
            pltpu.VMEM((chunks, bands, cap, rows, cells), bf16),
            pltpu.VMEM((bands, cap, cells), f32),
            pltpu.VMEM((bands, cap, cells), f32),
            pltpu.VMEM((chunks, slots + 1, rows, cells), f32),
            pltpu.VMEM((slots + 8, cells), f32),
            pltpu.VMEM((chunks, tiles, rows, cells), bf16),
            pltpu.VMEM((chunks, tiles, rows, cells), bf16),
            pltpu.VMEM((tiles, cells), f32),
            pltpu.VMEM((tiles, cells), f32),
            dma((chunks, bands)),
            dma((chunks, bands)),
            dma((bands,)),
            dma((bands,)),
            dma((chunks + 1,)),
            dma((chunks + 1,)),
        ],
        compiler_params=pltpu.CompilerParams(
            collective_id=0, has_side_effects=True, vmem_limit_bytes=60 * 1024 * 1024
        ),
        name="exchange",
    )(src, prev, last, partial, covered, keep)


def per_device(land_values, area_weights, land_mask, dest_band, dest_tile, ocean_mask):
    blocks_here = area_weights.shape[0]
    tile_cells = area_weights.shape[2]
    bands = lax.axis_size("band")
    halves = lax.axis_size("sub")
    half = lax.axis_index("sub")
    cap = max(2, 2 * blocks_here // bands)
    slots = bands * cap
    tiles = ocean_mask.shape[0] // tile_cells

    target = dest_band[:, 0]
    order = jnp.arange(blocks_here, dtype=jnp.int32)
    earlier = (target[:, None] == target[None, :]) & (order[None, :] < order[:, None])
    slot_of = target * cap + jnp.sum(earlier.astype(jnp.int32), axis=1)
    slot_ids = jnp.arange(slots, dtype=jnp.int32)
    packing = (slot_ids[:, None] == slot_of[None, :]).astype(jnp.int32)
    src = jnp.sum(packing * order[None, :], axis=1)
    tile_sent = jnp.sum(packing * (dest_tile + 1)[None, :], axis=1) - 1
    tile_recv = lax.all_to_all(
        tile_sent.reshape(bands, cap), "band", split_axis=0, concat_axis=0, tiled=True
    ).reshape(slots)

    partial, covered = block_products(land_values, area_weights, land_mask[None, :])

    same = (tile_recv[:, None] == tile_recv[None, :]) & (slot_ids[None, :] < slot_ids[:, None])
    prev = jnp.max(jnp.where(same, slot_ids[None, :], -1), axis=1)
    prev = jnp.where(prev < 0, slots, prev)
    listed = jnp.arange(halves * tiles, dtype=jnp.int32)
    listed = lax.rem(listed + (1 - half) * tiles, halves * tiles)
    hit = listed[:, None] == tile_recv[None, :]
    last = jnp.max(jnp.where(hit, slot_ids[None, :], -1), axis=1)
    last = jnp.where(last < 0, slots, last)

    keep = ocean_mask.reshape(tiles, tile_cells).astype(jnp.float32)
    return exchange(bands, cap, src, prev, last, partial, covered, keep)


def solution(mesh):
    in_specs = (
        P(None, ("band", "sub")),
        P(("band", "sub"), None, None),
        P(("band", "sub")),
        P(("band", "sub"), None),
        P(("band", "sub")),
        P(("band", "sub")),
    )
    out_specs = P(None, ("band", "sub"))
    return jax.shard_map(
        per_device, mesh=mesh, in_specs=in_specs, out_specs=out_specs, check_vma=False
    )
```

```python
import functools

import jax
import jax.numpy as jnp
from jax import lax
from jax.experimental import pallas as pl
from jax.experimental.pallas import tpu as pltpu
from jax.sharding import PartitionSpec as P

cover_floor = 0.5
ROWS = 8
LANES = 128
MESH = pl.DeviceIdType.MESH


def target_of(me, k, bands):
    if bands & (bands - 1):
        return lax.rem(me + k, bands)
    peer, bit = 0, 1
    while bit < bands:
        peer = peer + bit * lax.rem(me // bit + k // bit, 2)
        bit *= 2
    return peer


def greet_bands(barrier, me, bands):
    @pl.loop(1, bands)
    def _(k):
        pl.semaphore_signal(
            barrier, inc=1, device_id={"band": target_of(me, k, bands)}, device_id_type=MESH
        )


def block_kernel(
    group, chunks, bands, v_ref, w_ref, m_ref, t_ref, p_ref, c_ref, r_ref,
    landed, send_sem, recv_sem,
):
    me = lax.axis_index("band")
    cells = w_ref.shape[1]

    def index_copy(k):
        d = target_of(me, k, bands)
        return pltpu.make_async_remote_copy(
            src_ref=t_ref.at[d], dst_ref=landed.at[k],
            send_sem=send_sem.at[k], recv_sem=recv_sem.at[k],
            device_id={"band": d}, device_id_type=MESH,
        )

    @pl.when(pl.program_id(0) == 0)
    def _():
        barrier = pltpu.get_barrier_semaphore()
        greet_bands(barrier, me, bands)
        pl.semaphore_wait(barrier, bands - 1)

        @pl.loop(1, bands)
        def _(k):
            index_copy(k).start()

    for j in range(group):
        lanes = pl.ds(j * cells, cells)
        mb = m_ref[:, lanes].astype(jnp.float32).astype(jnp.bfloat16)
        lhs = jnp.concatenate(
            [v_ref[:, lanes] * mb, jnp.broadcast_to(mb, (16, cells))], axis=0
        )
        p = jnp.dot(lhs, w_ref[j], preferred_element_type=jnp.float32)
        for c in range(chunks):
            p_ref[c, j] = p[c * ROWS:(c + 1) * ROWS].astype(jnp.bfloat16)
        c_ref[pl.ds(j, 1), :] = (
            p[chunks * ROWS:chunks * ROWS + 1].astype(jnp.bfloat16).astype(jnp.float32)
        )

    @pl.when(pl.program_id(0) == pl.num_programs(0) - 1)
    def _():
        @pl.loop(1, bands)
        def _(k):
            index_copy(k).wait_send()
            index_copy(k).wait_recv()

        r_ref[0] = t_ref[me]
        r_ref[pl.ds(1, bands - 1)] = landed[pl.ds(1, bands - 1)]


def block_products(bands, values, weights, mask, tile_sent):
    fields = values.shape[0]
    blocks, cells, out_cells = weights.shape
    chunks = fields // ROWS
    group = 16
    return pl.pallas_call(
        functools.partial(block_kernel, group, chunks, bands),
        grid=(blocks // group,),
        in_specs=[
            pl.BlockSpec((fields, group * cells), lambda i: (0, i)),
            pl.BlockSpec((group, cells, out_cells), lambda i: (i, 0, 0)),
            pl.BlockSpec((1, group * cells), lambda i: (0, i)),
            pl.BlockSpec(memory_space=pltpu.VMEM),
        ],
        out_specs=[
            pl.BlockSpec((chunks, group, ROWS, out_cells), lambda i: (0, i, 0, 0)),
            pl.BlockSpec((group, out_cells), lambda i: (i, 0)),
            pl.BlockSpec(memory_space=pltpu.VMEM),
        ],
        out_shape=[
            jax.ShapeDtypeStruct((chunks, blocks, ROWS, out_cells), jnp.bfloat16),
            jax.ShapeDtypeStruct((blocks, out_cells), jnp.float32),
            jax.ShapeDtypeStruct(tile_sent.shape, jnp.int32),
        ],
        scratch_shapes=[
            pltpu.VMEM(tile_sent.shape, jnp.int32),
            pltpu.SemaphoreType.DMA((bands,)),
            pltpu.SemaphoreType.DMA((bands,)),
        ],
        compiler_params=pltpu.CompilerParams(collective_id=1, has_side_effects=True),
        name="block_products",
    )(values, weights, mask, tile_sent)


def exchange_kernel(
    bands, cap, chunks, tiles,
    src_ref, prev_ref, last_ref, p_ref, c_ref, wet_ref, out_ref,
    send, recv, csend, crecv, run, crun, xsend, xrecv, cxsend, cxrecv, done,
    send_sem, recv_sem, csend_sem, crecv_sem, xsend_sem, xrecv_sem, out_sem,
):
    me = lax.axis_index("band")
    half = lax.axis_index("sub")
    slots = bands * cap
    cells = xsend.shape[3]
    other = {"sub": 1 - half}
    step = 8

    barrier = pltpu.get_barrier_semaphore()
    greet_bands(barrier, me, bands)
    pl.semaphore_signal(barrier, inc=1, device_id=other, device_id_type=MESH)
    pl.semaphore_wait(barrier, bands)

    def chunk_copy(c, k):
        return pltpu.make_async_remote_copy(
            src_ref=send.at[c, k], dst_ref=recv.at[c, k],
            send_sem=send_sem.at[c, k], recv_sem=recv_sem.at[c, k],
            device_id={"band": target_of(me, k, bands)}, device_id_type=MESH,
        )

    def cover_copy(k):
        return pltpu.make_async_remote_copy(
            src_ref=csend.at[k], dst_ref=crecv.at[k],
            send_sem=csend_sem.at[k], recv_sem=crecv_sem.at[k],
            device_id={"band": target_of(me, k, bands)}, device_id_type=MESH,
        )

    def half_copy(c):
        return pltpu.make_async_remote_copy(
            src_ref=xsend.at[c], dst_ref=xrecv.at[c],
            send_sem=xsend_sem.at[c], recv_sem=xrecv_sem.at[c],
            device_id=other, device_id_type=MESH,
        )

    half_cover = pltpu.make_async_remote_copy(
        src_ref=cxsend, dst_ref=cxrecv,
        send_sem=xsend_sem.at[chunks], recv_sem=xrecv_sem.at[chunks],
        device_id=other, device_id_type=MESH,
    )

    def out_copy(c):
        return pltpu.make_async_copy(
            done.at[c % 2], out_ref.at[pl.ds(c * ROWS, ROWS), :], out_sem.at[c % 2]
        )

    def each_tile(body):
        @pl.loop(0, tiles // step)
        def _(g):
            for u in range(step):
                body(g * step + u)

    def finish(c):
        half_copy(c).wait_recv()
        if c >= 2:
            out_copy(c - 2).wait()

        def one(t):
            total = run[c, last_ref[tiles + t]] + xrecv[c, t].astype(jnp.float32)
            lanes = pl.ds(pl.multiple_of(t * cells, cells), cells)
            done[c % 2, :, lanes] = total * cxrecv[pl.ds(t, 1), :]

        each_tile(one)
        out_copy(c).start()

    def send_chunk(c):
        @pl.loop(1, bands)
        def _(k):
            d = target_of(me, k, bands)
            for j in range(cap):
                send[c, k, j] = p_ref[c, src_ref[d * cap + j]]
            chunk_copy(c, k).start()

        for j in range(cap):
            recv[c, 0, j] = p_ref[c, src_ref[me * cap + j]]

    send_chunk(0)

    @pl.loop(1, bands)
    def _(k):
        d = target_of(me, k, bands)
        for j in range(cap):
            csend[k, pl.ds(j, 1), :] = c_ref[pl.ds(src_ref[d * cap + j], 1), :]
        cover_copy(k).start()

    for j in range(cap):
        crecv[0, pl.ds(j, 1), :] = c_ref[pl.ds(src_ref[me * cap + j], 1), :]

    for c in range(1, chunks):
        send_chunk(c)

    for c in range(chunks):
        run[c, slots] = jnp.zeros(run.shape[2:], jnp.float32)

        def add(k, c=c):
            for j in range(cap):
                i = k * cap + j
                run[c, i] = run[c, prev_ref[i]] + recv[c, k, j].astype(jnp.float32)

        add(0)

        @pl.loop(1, bands)
        def _(k, c=c):
            chunk_copy(c, k).wait_recv()
            add(k)

        def give(t, c=c):
            xsend[c, t] = run[c, last_ref[t]].astype(jnp.bfloat16)

        each_tile(give)
        half_copy(c).start()

        if c == 0:
            @pl.loop(1, bands)
            def _(k):
                cover_copy(k).wait_recv()

            crun[pl.ds(slots, 8), :] = jnp.zeros((8, cells), jnp.float32)

            @pl.loop(0, bands)
            def _(k):
                for j in range(cap):
                    i = k * cap + j
                    crun[pl.ds(i, 1), :] = (
                        crun[pl.ds(prev_ref[i], 1), :] + crecv[k, pl.ds(j, 1), :]
                    )

            def give_cover(t):
                cxsend[pl.ds(t, 1), :] = crun[pl.ds(last_ref[t], 1), :]

            each_tile(give_cover)
            half_cover.start()

        if c == 1:
            half_cover.wait_recv()

            def factor(t):
                row = pl.ds(t, 1)
                total = crun[pl.ds(last_ref[tiles + t], 1), :] + cxrecv[row, :]
                wet = wet_ref[row, :].astype(jnp.float32)
                cxrecv[row, :] = wet / jnp.maximum(total, cover_floor)

            each_tile(factor)

        if c >= 1:
            finish(c - 1)

    finish(chunks - 1)

    half_cover.wait_send()
    for c in range(chunks):
        half_copy(c).wait_send()

    @pl.loop(1, bands)
    def _(k):
        cover_copy(k).wait_send()
        for c in range(chunks):
            chunk_copy(c, k).wait_send()

    for c in range(max(0, chunks - 2), chunks):
        out_copy(c).wait()


def exchange(bands, cap, src, prev, last, partial, covered, wet):
    chunks, _, rows, cells = partial.shape
    tiles = wet.shape[0]
    slots = bands * cap
    smem = pl.BlockSpec(memory_space=pltpu.SMEM)
    vmem = pl.BlockSpec(memory_space=pltpu.VMEM)
    bf16, f32 = jnp.bfloat16, jnp.float32
    dma = pltpu.SemaphoreType.DMA
    return pl.pallas_call(
        functools.partial(exchange_kernel, bands, cap, chunks, tiles),
        in_specs=[smem, smem, smem, vmem, vmem, vmem],
        out_specs=pl.BlockSpec(memory_space=pl.ANY),
        out_shape=jax.ShapeDtypeStruct((chunks * rows, tiles * cells), f32),
        scratch_shapes=[
            pltpu.VMEM((chunks, bands, cap, rows, cells), bf16),
            pltpu.VMEM((chunks, bands, cap, rows, cells), bf16),
            pltpu.VMEM((bands, cap, cells), f32),
            pltpu.VMEM((bands, cap, cells), f32),
            pltpu.VMEM((chunks, slots + 1, rows, cells), f32),
            pltpu.VMEM((slots + 8, cells), f32),
            pltpu.VMEM((chunks, tiles, rows, cells), bf16),
            pltpu.VMEM((chunks, tiles, rows, cells), bf16),
            pltpu.VMEM((tiles, cells), f32),
            pltpu.VMEM((tiles, cells), f32),
            pltpu.VMEM((2, rows, tiles * cells), f32),
            dma((chunks, bands)),
            dma((chunks, bands)),
            dma((bands,)),
            dma((bands,)),
            dma((chunks + 1,)),
            dma((chunks + 1,)),
            dma((2,)),
        ],
        compiler_params=pltpu.CompilerParams(
            collective_id=0, has_side_effects=True, vmem_limit_bytes=60 * 1024 * 1024
        ),
        name="exchange",
    )(src, prev, last, partial, covered, wet)


def per_device(land_values, area_weights, land_mask, dest_band, dest_tile, ocean_mask):
    blocks_here = area_weights.shape[0]
    tile_cells = area_weights.shape[2]
    bands = lax.axis_size("band")
    halves = lax.axis_size("sub")
    half = lax.axis_index("sub")
    cap = max(2, 2 * blocks_here // bands)
    slots = bands * cap
    tiles = ocean_mask.shape[0] // tile_cells

    target = dest_band[:, 0]
    order = jnp.arange(blocks_here, dtype=jnp.int32)
    earlier = (target[:, None] == target[None, :]) & (order[None, :] < order[:, None])
    slot_of = target * cap + jnp.sum(earlier.astype(jnp.int32), axis=1)
    slot_ids = jnp.arange(slots, dtype=jnp.int32)
    packing = (slot_ids[:, None] == slot_of[None, :]).astype(jnp.int32)
    src = jnp.sum(packing * order[None, :], axis=1)
    tile_sent = jnp.sum(packing * (dest_tile + 1)[None, :], axis=1) - 1
    tile_sent = jnp.pad(
        tile_sent.reshape(bands, 1, cap), ((0, 0), (0, 0), (0, LANES - cap)), constant_values=-1
    )

    partial, covered, tile_recv = block_products(
        bands, land_values, area_weights, land_mask[None, :], tile_sent
    )
    tile_recv = tile_recv[:, 0, :cap].reshape(slots)

    same = (tile_recv[:, None] == tile_recv[None, :]) & (slot_ids[None, :] < slot_ids[:, None])
    prev = jnp.max(jnp.where(same, slot_ids[None, :], -1), axis=1)
    prev = jnp.where(prev < 0, slots, prev)
    listed = jnp.arange(halves * tiles, dtype=jnp.int32)
    listed = lax.rem(listed + (1 - half) * tiles, halves * tiles)
    hit = listed[:, None] == tile_recv[None, :]
    last = jnp.max(jnp.where(hit, slot_ids[None, :], -1), axis=1)
    last = jnp.where(last < 0, slots, last)

    wet = ocean_mask.reshape(tiles, tile_cells)
    return exchange(bands, cap, src, prev, last, partial, covered, wet)


def solution(mesh):
    in_specs = (
        P(None, ("band", "sub")),
        P(("band", "sub"), None, None),
        P(("band", "sub")),
        P(("band", "sub"), None),
        P(("band", "sub")),
        P(("band", "sub")),
    )
    out_specs = P(None, ("band", "sub"))
    return jax.shard_map(
        per_device, mesh=mesh, in_specs=in_specs, out_specs=out_specs, check_vma=False
    )
```
